128 devices in a mesh: scen: 8 (over x_hi, y), slab: 16 (over z, x_lo, core).
Axes of the slice: x: 4 (x_hi: 2, x_lo: 2; x = x_hi * 2 + x_lo), y: 4, z: 4, core: 2. Of those that a mesh axis runs over, the one named last changes fastest.
Arguments:
- start: float32 [8, 128, 256, 256], P('scen', 'slab'), may hold values from 0 to 2
- flow_east: float32 [8, 128, 256, 256], P('scen', 'slab'), may hold values from 0.3 to 1.2
- flow_north: float32 [8, 128, 256, 256], P('scen', 'slab'), may hold values from 0.3 to 1.2
- wells: int32 [128, 256, 256], P('slab'), may hold values 0 or 1
- monitors: int32 [128, 256, 256], P('slab'), may hold values 0 or 1
- control: float32 [8, 32, 4096], P('scen', 'slab'), may hold values from -3 to 3
- multiplier: float32 [8, 32, 4096], P('scen', 'slab'), may hold values from -3 to 3
- threshold: float32 [1], replicated, may hold values from 0.8 to 1.3
Outputs:
- final_fields: float32 [8, 128, 256, 256], P('scen', 'slab')
- consensus_next: float32 [32, 4096], P('slab')
- multiplier_next: float32 [8, 32, 4096], P('scen', 'slab')
- cvar: float32 [1], replicated
The draws below stay inside these ranges and needn't reach their ends.
All inputs are finite; a program needn't handle non-finite values. No bound on the sum of `wells` or of `monitors` on one device may be relied on, other than what follows from the above.
Results may differ from the reference program's by a relative error of at most 0.00002.
Values sent between devices are 32-bit elements; how exact they have to be, the bound alone decides.
No kernel may reach another device: no remote copies, remote signals or barrier semaphores. Data moves between devices by JAX's collectives and lax.ppermute only.
A program may use at most 192 MiB of HBM per device.

```python
import jax
import jax.numpy as jnp
from jax import lax

NX = 256
NY = 256
STEPS = 4
SCEN = 8
NZ = 128
NZC = 32
CC = 4096


def plant(drawn, stream_key, smallest, largest):
    longest = drawn.shape.index(max(drawn.shape))
    spots = []
    for shift in (0, 1):
        where = [jax.random.randint(jax.random.fold_in(stream_key, axis), (), 0, length) for axis, length in enumerate(drawn.shape)]
        where[longest] = (where[longest] + shift) % drawn.shape[longest]
        spots.append(tuple(where))
    return drawn.at[spots[0]].set(smallest).at[spots[1]].set(largest)


def block_scale(rng, shape, split, least, high):
    def one(position, blocks):
        heights = jax.random.uniform(jax.random.fold_in(jax.random.fold_in(rng, 6), position), (blocks,), jnp.float32, least / len(split), high / len(split))
        return jnp.repeat(jnp.exp(heights), shape[position] // blocks).reshape((-1,) + (1,) * (len(shape) - position - 1))

    factor_of = one(*split[0])
    for cut in split[1:]:
        factor_of = factor_of * one(*cut)
    return factor_of


def noise(own_key, dims, width, bound, split=(), held_as=jnp.bfloat16):
    entries = jax.random.normal(own_key, dims, jnp.float32) * width
    if len(split) > 0:
        entries = block_scale(own_key, dims, split, -0.22, 0.18) * entries
    return jnp.clip(entries, min=-bound, max=bound).astype(held_as)


def setup_inputs(seed: int = 0) -> dict:
    keys = jax.random.split(jax.random.key(seed), 9)
    return {
        "start": jnp.clip(2.0 * jax.random.uniform(keys[0], (SCEN, NZ, NX, NY), jnp.float32) ** block_scale(keys[0], (SCEN, NZ, NX, NY), ((0, 8), (1, 16)), -0.2, 0.2), 0.0, 2.0),
        "flow_east": jnp.clip(0.3 + 0.90000004 * jax.random.uniform(keys[1], (SCEN, NZ, NX, NY), jnp.float32) ** block_scale(keys[1], (SCEN, NZ, NX, NY), ((0, 8), (1, 16)), -0.2, 0.2), 0.3, 1.2),
        "flow_north": jnp.clip(0.3 + 0.90000004 * jax.random.uniform(keys[2], (SCEN, NZ, NX, NY), jnp.float32) ** block_scale(keys[2], (SCEN, NZ, NX, NY), ((0, 8), (1, 16)), -0.2, 0.2), 0.3, 1.2),
        "wells": plant((jax.random.randint(keys[3], (NZ, NX, NY), 0, 4) < 1).astype(jnp.int32), jax.random.fold_in(keys[3], 1), 0, 1),
        "monitors": plant((jax.random.randint(keys[4], (NZ, NX, NY), 0, 4) < 1).astype(jnp.int32), jax.random.fold_in(keys[4], 1), 0, 1),
        "control": noise(keys[5], (SCEN, NZC, CC), 0.5, 3.0, ((0, 8), (1, 16)), jnp.float32),
        "multiplier": noise(keys[6], (SCEN, NZC, CC), 0.5, 3.0, ((0, 8), (1, 16)), jnp.float32),
        "threshold": jnp.clip(jax.random.uniform(keys[7], (1,), jnp.float32, 0.8, 1.3), 0.8, 1.3),
    }


EPS_LIMIT = 0.01
TIME_STEP = 0.25
DIFF_FLAT = 0.1
DIFF_VERTICAL = 0.25
BETA_LEVEL = 0.75
SOFT_WIDTH = 0.25

def pad_axis(field, which_axis, low_pad, high_pad):
    widths = [(0, 0)] * field.ndim
    widths[which_axis] = (low_pad, high_pad)
    return jnp.pad(field, widths)

def second_difference(padded, field, which_axis):
    length = field.shape[which_axis]
    upper_cells = lax.slice_in_dim(padded, 2, length + 2, axis=which_axis)
    lower_cells = lax.slice_in_dim(padded, 0, length, axis=which_axis)
    return upper_cells - 2.0 * field + lower_cells

def divergence(field, velocity, which_axis):
    length = field.shape[which_axis]
    padded = pad_axis(field, which_axis, 1, 1)
    lower_cells = lax.slice_in_dim(padded, 0, length, axis=which_axis)
    upper_cells = lax.slice_in_dim(padded, 2, length + 2, axis=which_axis)
    backward = field - lower_cells
    forward = upper_cells - field
    product = backward * forward
    weight = (product + jnp.sqrt(product * product + EPS_LIMIT * EPS_LIMIT)) / (backward * backward + forward * forward + EPS_LIMIT)
    face_value = field + 0.5 * weight * (backward / 3.0 + 2.0 * forward / 3.0)
    fluxes = velocity * face_value
    previous = lax.slice_in_dim(pad_axis(fluxes, which_axis, 1, 0), 0, length, axis=which_axis)
    return fluxes - previous

def horizontal(field, flow_east, flow_north, rate):
    advect = divergence(field, flow_east, 1) + divergence(field, flow_north, 2)
    spread = second_difference(pad_axis(field, 1, 1, 1), field, 1) + second_difference(pad_axis(field, 2, 1, 1), field, 2)
    return -advect + DIFF_FLAT * spread - rate * field

def prolong(coarse, row_count, column_count):
    plane_count = coarse.shape[0]
    cube = coarse.reshape(plane_count, 1, row_count // 4, 1, column_count // 4, 1)
    cube = jnp.broadcast_to(cube, (plane_count, 4, row_count // 4, 4, column_count // 4, 4))
    return cube.reshape(plane_count * 4, row_count, column_count)

def restrict(fine):
    plane_count, row_count, column_count = fine.shape
    blocks = fine.reshape(plane_count // 4, 4, row_count // 4, 4, column_count // 4, 4).sum(axis=(1, 3, 5))
    return blocks.reshape(plane_count // 4, row_count // 4 * (column_count // 4))

def forward_run(start, flow_east, flow_north, rate):
    field = start
    for step_index in range(STEPS):
        vertical = second_difference(pad_axis(field, 0, 1, 1), field, 0)
        field = field + TIME_STEP * (horizontal(field, flow_east, flow_north, rate) + DIFF_VERTICAL * vertical)
    return field

def reference(start, flow_east, flow_north, wells, monitors, control, multiplier, threshold):
    consensus = lax.optimization_barrier(jnp.sum(control + multiplier, axis=0)) / SCEN
    wells_float = wells.astype(jnp.float32)
    monitor_float = monitors.astype(jnp.float32)
    rate = wells_float * prolong(consensus, NX, NY)
    count = jnp.maximum(jnp.sum(monitor_float), 1.0)
    coarse_cells = NZ * NX * NY / 64.0

    def one_scenario(inputs):
        first, east, north = inputs
        final_field, pullback = jax.vjp(lambda rate_field: forward_run(first, east, north, rate_field), rate)
        loss = jnp.sum(monitor_float * final_field * final_field) / count
        scaled = (loss - threshold[0]) / SOFT_WIDTH
        weight = jax.nn.sigmoid(scaled) / ((1.0 - BETA_LEVEL) * SCEN)
        soft_term = SOFT_WIDTH * jax.nn.softplus(scaled) / ((1.0 - BETA_LEVEL) * SCEN)
        adjoint_start = weight * 2.0 * monitor_float * final_field / count
        rate_grad, = pullback(adjoint_start)
        gradient = coarse_cells * restrict(wells_float * rate_grad)
        return (final_field, soft_term, gradient)
    final_fields, soft_terms, gradients = lax.map(one_scenario, (start, flow_east, flow_north))
    consensus_next = consensus - lax.optimization_barrier(jnp.sum(gradients, axis=0))
    multiplier_next = multiplier + control - consensus_next[None]
    cvar = threshold + jnp.sum(soft_terms)
    return (final_fields, consensus_next, multiplier_next, cvar)
```

```python
import functools

import jax
import jax.numpy as jnp
from jax import lax
from jax.experimental import pallas as pl
from jax.experimental.pallas import tpu as pltpu
from jax.sharding import PartitionSpec as P

STEPS = 4
EPS_LIMIT = 0.01
TIME_STEP = 0.25
DIFF_FLAT = 0.1
DIFF_VERTICAL = 0.25
BETA_LEVEL = 0.75
SOFT_WIDTH = 0.25

NZ, NX, NY = 8, 256, 256
HP = NX + 8
ZP = 2 * HP
F0 = 8
ROWS = F0 + NZ * ZP + 8
SEG = HP // 8
VERT = TIME_STEP * DIFF_VERTICAL
KEEP = 1.0 - 2.0 * VERT
f32 = jnp.float32
VM = pl.BlockSpec(memory_space=pltpu.VMEM)
HBM = pl.BlockSpec(memory_space=pltpu.HBM)
FIELD = jax.ShapeDtypeStruct((ROWS, 128), f32)
PLANE = jax.ShapeDtypeStruct((NX, NY), f32)


def seg_load(ref, z, h, r):
    return ref[pl.ds(F0 + z * ZP + h * HP + r, 8, stride=SEG), :]


def seg_store(ref, z, h, r, value):
    ref[pl.ds(F0 + z * ZP + h * HP + r, 8, stride=SEG), :] = value


def block_rows(z, h, j):
    return pl.ds(pl.multiple_of(F0 + z * ZP + h * HP + 8 * j, 8), 8)


def zero_pads(ref):
    zeros = jnp.zeros((8, 128), f32)
    ref[0:8, :] = zeros
    ref[ROWS - 8 : ROWS, :] = zeros
    for z in range(NZ):
        for h in range(2):
            start = F0 + z * ZP + h * HP + NX
            ref[start : start + 8, :] = zeros


def limiter(b, f, sb, sf):
    p = b * f
    q = p * p + EPS_LIMIT * EPS_LIMIT
    s = q * lax.rsqrt(q)
    r = lax.rsqrt(sb + sf + EPS_LIMIT)
    w = (p + s) * (r * r)
    return w * (b * (1.0 / 6.0) + f * (1.0 / 3.0))


def limiter_slopes(b, f, sb, sf):
    p = b * f
    q = p * p + EPS_LIMIT * EPS_LIMIT
    rs = lax.rsqrt(q)
    s = q * rs
    r = lax.rsqrt(sb + sf + EPS_LIMIT)
    r = r * r
    w = (p + s) * r
    u = b * (1.0 / 6.0) + f * (1.0 / 3.0)
    r2 = r + r
    slope_b = (f * rs - b * r2) * u + (1.0 / 6.0)
    slope_f = (b * rs - f * r2) * u + (1.0 / 3.0)
    return w, slope_b, slope_f


def lane_masks():
    lane = lax.broadcasted_iota(jnp.int32, (8, 128), 1)
    sub = lax.broadcasted_iota(jnp.int32, (8, 128), 0)
    return lane == 0, lane == 127, sub < 7


def from_left(pair, first, edge):
    rolled = [pltpu.roll(v, 1, 1) for v in pair]
    return [jnp.where(edge, first, rolled[0]), jnp.where(edge, rolled[0], rolled[1])]


def from_right(pair, last, edge):
    rolled = [pltpu.roll(v, 127, 1) for v in pair]
    return [jnp.where(edge, rolled[1], rolled[0]), jnp.where(edge, last, rolled[1])]


def forward_planes(z, unroll, c_ref, ve_ref, vn_ref, co_ref, out_ref):
    at_first, at_last, inside = lane_masks()
    below = jnp.maximum(z - 1, 0)
    above = jnp.minimum(z + 1, NZ - 1)
    has_below = jnp.where(z > 0, VERT, 0.0)
    has_above = jnp.where(z < NZ - 1, VERT, 0.0)

    def flux(v, c, b, f, sb, sf):
        return v * (c + limiter(b, f, sb, sf)) - DIFF_FLAT * f

    def one(r, c, b, sb, before):
        after = [seg_load(c_ref, z, h, r + 1) for h in (0, 1)]
        left = from_left(c, 0.0, at_first)
        right = from_right(c, 0.0, at_last)
        f, sf, gx, gy = [], [], [], []
        for h in (0, 1):
            fx = after[h] - c[h]
            sx = fx * fx
            gx.append(flux(seg_load(ve_ref, z, h, r), c[h], b[h], fx, sb[h], sx))
            by = c[h] - left[h]
            fy = right[h] - c[h]
            gy.append(flux(seg_load(vn_ref, z, h, r), c[h], by, fy, by * by, fy * fy))
            f.append(fx)
            sf.append(sx)
        gl = from_left(gy, -DIFF_FLAT * c[0], at_first)
        for h in (0, 1):
            vertical = has_below * seg_load(c_ref, below, h, r) + has_above * seg_load(c_ref, above, h, r)
            keep = KEEP if co_ref is None else seg_load(co_ref, z, h, r)
            out = keep * c[h] + vertical - TIME_STEP * ((gx[h] - before[h]) + (gy[h] - gl[h]))
            seg_store(out_ref, z, h, r, jnp.where(inside | (r < NX - 7 * SEG), out, 0.0))
        return after, f, sf, gx

    c, b, sb, before = [], [], [], []
    for h in (0, 1):
        m2 = seg_load(c_ref, z, h, -2)
        m1 = seg_load(c_ref, z, h, -1)
        c0 = seg_load(c_ref, z, h, 0)
        bm = m1 - m2
        fm = c0 - m1
        sm = fm * fm
        before.append(flux(seg_load(ve_ref, z, h, -1), m1, bm, fm, bm * bm, sm))
        c.append(c0)
        b.append(fm)
        sb.append(sm)

    def block(i, carry):
        for j in range(unroll):
            carry = one(i * unroll + j, *carry)
        return carry

    lax.fori_loop(0, SEG // unroll, block, (c, b, sb, before))


def first_kernel(start_ref, east_ref, north_ref, c_ref, ve_ref, vn_ref, out_ref, sem):
    def copies(z):
        made = []
        for source, target in ((start_ref, c_ref), (east_ref, ve_ref), (north_ref, vn_ref)):
            for h in (0, 1):
                made.append(
                    pltpu.make_async_copy(
                        source.at[0, z, :, pl.ds(h * 128, 128)],
                        target.at[pl.ds(pl.multiple_of(F0 + z * ZP + h * HP, 8), NX), :],
                        sem.at[z, len(made)],
                    )
                )
        return made

    for z in range(NZ):
        for copy in copies(z):
            copy.start()
    for ref in (c_ref, ve_ref, vn_ref, out_ref):
        zero_pads(ref)
    for copy in copies(0):
        copy.wait()

    def plane(z, unused):
        @pl.when(z < NZ - 1)
        def _():
            for copy in copies(z + 1):
                copy.wait()

        forward_planes(z, 11, c_ref, ve_ref, vn_ref, None, out_ref)
        return unused

    lax.fori_loop(0, NZ, plane, 0)


def step_kernel(c_ref, ve_ref, vn_ref, co_ref, out_ref):
    zero_pads(out_ref)

    def plane(z, unused):
        forward_planes(z, 11, c_ref, ve_ref, vn_ref, co_ref, out_ref)
        return unused

    lax.fori_loop(0, NZ, plane, 0)


def facing():
    z_chip = jnp.where(lax.axis_index("slab") % 2 == 0, NZ - 1, 0)
    return z_chip, NZ - 1 - z_chip


def fix_planes(chip_ref, near_ref, field_ref, target_ref, send_chip_ref, send_near_ref):
    z_chip, z_near = facing()

    def block(j, unused):
        for h in (0, 1):
            lanes = slice(h * 128, h * 128 + 128)
            rows = pl.ds(pl.multiple_of(8 * j, 8), 8)
            for z, halo_ref, send_ref in ((z_chip, chip_ref, send_chip_ref), (z_near, near_ref, send_near_ref)):
                value = field_ref[block_rows(z, h, j), :] + VERT * halo_ref[rows, lanes]
                target_ref[block_rows(z, h, j), :] = value
                if send_ref is not None:
                    send_ref[rows, lanes] = value
        return unused

    lax.fori_loop(0, NX // 8, block, 0, unroll=4)


def fix_kernel(chip_ref, near_ref, field_ref, out_ref, send_chip_ref, send_near_ref):
    fix_planes(chip_ref, near_ref, field_ref, out_ref, send_chip_ref, send_near_ref)


def send_planes(field_ref, send_chip_ref, send_near_ref):
    z_chip, z_near = facing()

    def block(j, unused):
        for h in (0, 1):
            lanes = slice(h * 128, h * 128 + 128)
            rows = pl.ds(pl.multiple_of(8 * j, 8), 8)
            send_chip_ref[rows, lanes] = field_ref[block_rows(z_chip, h, j), :]
            send_near_ref[rows, lanes] = field_ref[block_rows(z_near, h, j), :]
        return unused

    lax.fori_loop(0, NX // 8, block, 0, unroll=4)


def mask_copies(mask_hbm, mask_ref, sem):
    return [
        pltpu.make_async_copy(mask_hbm.at[z], mask_ref.at[z], sem.at[z]) for z in range(NZ)
    ]


def rate_kernel(chip_ref, near_ref, field_ref, c0_ref, cons_ref, wells_hbm, out_ref, send_chip_ref, send_near_ref, co_ref, wells_ref, sem):
    copies = mask_copies(wells_hbm, wells_ref, sem)
    for copy in copies:
        copy.start()
    lane = lax.broadcasted_iota(jnp.int32, (8, 128), 1)
    sub = lax.broadcasted_iota(jnp.int32, (8, 128), 0)
    base = jnp.where(sub < 4, 0, 64) + lane // 4
    zero_pads(co_ref)
    for copy in copies:
        copy.wait()

    def block(j, unused):
        for h in (0, 1):
            for p in (0, 1):
                coarse = cons_ref[pl.ds(p, 1), pl.ds(pl.multiple_of(j * 128, 128), 128)]
                wide = jnp.broadcast_to(coarse * TIME_STEP, (8, 128))
                wide = jnp.take_along_axis(wide, base + 32 * h, axis=1)
                for z in range(4 * p, 4 * p + 4):
                    wells = wells_ref[z, pl.ds(pl.multiple_of(8 * j, 8), 8), h * 128 : h * 128 + 128]
                    rate = wells.astype(f32) * wide
                    at = block_rows(z, h, j)
                    co_ref[at, :] = KEEP - rate
                    out_ref[at, :] = field_ref[at, :] - rate * c0_ref[at, :]
        return unused

    lax.fori_loop(0, NX // 8, block, 0)
    fix_planes(chip_ref, near_ref, out_ref, out_ref, send_chip_ref, send_near_ref)


def seed_kernel(chip_ref, near_ref, ahead_ref, monitors_hbm, final_hbm, adjoint_ref, send_chip_ref, send_near_ref, sums_ref, field_ref, c_ref, monitors_ref, sem, out_sem):
    copies = mask_copies(monitors_hbm, monitors_ref, sem)
    for copy in copies:
        copy.start()
    zero_pads(adjoint_ref)
    fix_planes(chip_ref, near_ref, ahead_ref, field_ref, None, None)
    for copy in copies:
        copy.wait()

    def block(j, sums):
        mass, count = sums
        for z in range(NZ):
            for h in (0, 1):
                rows = pl.ds(pl.multiple_of(8 * j, 8), 8)
                value = field_ref[block_rows(z, h, j), :]
                c_ref[z, rows, h * 128 : h * 128 + 128] = value
                monitor = monitors_ref[z, rows, h * 128 : h * 128 + 128].astype(f32)
                seed = monitor * value
                adjoint_ref[block_rows(z, h, j), :] = seed
                mass = mass + seed * value
                count = count + monitor
        return mass, count

    zeros = jnp.zeros((8, 128), f32)
    mass, count = lax.fori_loop(0, NX // 8, block, (zeros, zeros))
    out = pltpu.make_async_copy(c_ref, final_hbm.at[0], out_sem)
    out.start()
    sums_ref[0:8, :] = jnp.broadcast_to(jnp.sum(jnp.sum(mass, axis=0, keepdims=True), axis=1, keepdims=True), (8, 128))
    sums_ref[8:16, :] = jnp.broadcast_to(jnp.sum(jnp.sum(count, axis=0, keepdims=True), axis=1, keepdims=True), (8, 128))
    send_planes(adjoint_ref, send_chip_ref, send_near_ref)
    out.wait()


def adjoint_planes(z, unroll, c_ref, a_ref, ve_ref, vn_ref, co_ref, rg_in_ref, out_ref, rg_ref):
    at_first, at_last, inside = lane_masks()
    below = jnp.maximum(z - 1, 0)
    above = jnp.minimum(z + 1, NZ - 1)
    has_below = jnp.where(z > 0, VERT, 0.0)
    has_above = jnp.where(z < NZ - 1, VERT, 0.0)

    def parts(v, g, b, f, sb, sf):
        w, slope_b, slope_f = limiter_slopes(b, f, sb, sf)
        direct = v * g
        scaled = direct * w
        return direct, scaled * slope_b, scaled * slope_f - DIFF_FLAT * g

    def along_x(r, c, b, sb, a):
        after = [seg_load(c_ref, z, h, r + 1) for h in (0, 1)]
        next_a = [seg_load(a_ref, z, h, r + 1) for h in (0, 1)]
        f, sf, direct, back, front = [], [], [], [], []
        for h in (0, 1):
            fx = after[h] - c[h]
            sx = fx * fx
            d, k, n = parts(seg_load(ve_ref, z, h, r), next_a[h] - a[h], b[h], fx, sb[h], sx)
            f.append(fx)
            sf.append(sx)
            direct.append(d)
            back.append(k)
            front.append(n)
        return after, f, sf, next_a, direct, back, front

    def along_y(r, c, a):
        left = from_left(c, 0.0, at_first)
        right = from_right(c, 0.0, at_last)
        next_a = from_right(a, 0.0, at_last)
        direct, back, front = [], [], []
        for h in (0, 1):
            by = c[h] - left[h]
            fy = right[h] - c[h]
            d, k, n = parts(seg_load(vn_ref, z, h, r), next_a[h] - a[h], by, fy, by * by, fy * fy)
            direct.append(d)
            back.append(k)
            front.append(n)
        fl = from_left(front, -DIFF_FLAT * a[0], at_first)
        kr = from_right(back, 0.0, at_last)
        return [direct[h] + (back[h] - front[h]) + fl[h] - kr[h] for h in (0, 1)]

    def row(r, c, b, sb, a, before):
        after, f, sf, next_a, direct, back, front = along_x(r, c, b, sb, a)
        flat = along_y(r, c, a)
        pulled = []
        for h in (0, 1):
            vertical = has_below * seg_load(a_ref, below, h, r) + has_above * seg_load(a_ref, above, h, r)
            grad = c[h] * a[h]
            if rg_in_ref is not None:
                grad = grad + seg_load(rg_in_ref, z, h, r)
            seg_store(rg_ref, z, h, r, grad)
            here = flat[h] + direct[h] + (back[h] - front[h]) + before[h]
            pulled.append(seg_load(co_ref, z, h, r) * a[h] + vertical + TIME_STEP * here)
        return after, f, sf, next_a, front, back, pulled

    start_c, start_b, start_s, start_a = [], [], [], []
    for h in (0, 1):
        m2 = seg_load(c_ref, z, h, -2)
        m1 = seg_load(c_ref, z, h, -1)
        bm = m1 - m2
        start_c.append(m1)
        start_b.append(bm)
        start_s.append(bm * bm)
        start_a.append(seg_load(a_ref, z, h, -1))
    c, b, sb, a, _, _, before = along_x(-1, start_c, start_b, start_s, start_a)
    zeros = [jnp.zeros((8, 128), f32)] * 2

    def block(i, carry):
        c, b, sb, a, before, pulled = carry
        for j in range(unroll):
            r = i * unroll + j
            c, b, sb, a, before, back, new = row(r, c, b, sb, a, before)
            for h in (0, 1):
                out = pulled[h] - TIME_STEP * back[h]
                seg_store(out_ref, z, h, r - 1, jnp.where(inside | (r - 1 < NX - 7 * SEG), out, 0.0))
            pulled = new
        return c, b, sb, a, before, pulled

    c, b, sb, a, before, pulled = lax.fori_loop(0, SEG // unroll, block, (c, b, sb, a, before, zeros))
    last = along_x(SEG, c, b, sb, a)
    for h in (0, 1):
        out = pulled[h] - TIME_STEP * last[5][h]
        seg_store(out_ref, z, h, SEG - 1, jnp.where(inside, out, 0.0))


def adjoint_kernel(c_ref, a_ref, ve_ref, vn_ref, co_ref, *rest):
    rg_in_ref = rest[0] if len(rest) == 3 else None
    out_ref, rg_ref = rest[-2:]

    def plane(z, unused):
        adjoint_planes(z, 11, c_ref, a_ref, ve_ref, vn_ref, co_ref, rg_in_ref, out_ref, rg_ref)
        return unused

    lax.fori_loop(0, NZ, plane, 0)
    zero_pads(out_ref)


def restrict_kernel(chip_ref, near_ref, ahead_ref, c0_ref, rg_ref, wells_hbm, out_ref, field_ref, wide_ref, wells_ref, sem):
    copies = mask_copies(wells_hbm, wells_ref, sem)
    for copy in copies:
        copy.start()
    fix_planes(chip_ref, near_ref, ahead_ref, field_ref, None, None)
    for copy in copies:
        copy.wait()

    def block(j, unused):
        for h in (0, 1):
            for p in (0, 1):
                total = jnp.zeros((8, 128), f32)
                for z in range(4 * p, 4 * p + 4):
                    at = block_rows(z, h, j)
                    rows = pl.ds(pl.multiple_of(8 * j, 8), 8)
                    wells = wells_ref[z, rows, h * 128 : h * 128 + 128].astype(f32)
                    total = total + wells * (rg_ref[at, :] + c0_ref[at, :] * field_ref[at, :])
                wide_ref[p, pl.ds(pl.multiple_of(8 * j, 8), 8), h * 128 : h * 128 + 128] = total
        return unused

    lax.fori_loop(0, NX // 8, block, 0)
    fine = lax.broadcasted_iota(jnp.int32, (NY, 128), 0) // 4
    coarse = lax.broadcasted_iota(jnp.int32, (NY, 128), 1) % 64
    sums = jnp.where(fine == coarse, 1.0, 0.0).astype(f32)
    row = lax.broadcasted_iota(jnp.int32, (NX, 128), 0) % 8
    lane = lax.broadcasted_iota(jnp.int32, (NX, 128), 1)
    own = (row < 4) == (lane < 64)
    for p in (0, 1):
        part = jnp.dot(wide_ref[p], sums, precision=lax.Precision.HIGHEST, preferred_element_type=f32)
        part = jnp.where(own, part, 0.0).reshape(NX // 8, 8, 128).sum(axis=1)
        for j in range(NX // 8):
            out_ref[p : p + 1, j * 128 : (j + 1) * 128] = part[j : j + 1, :]


def call(kernel, name, flops, **kwargs):
    return pl.pallas_call(
        kernel,
        name=name,
        compiler_params=pltpu.CompilerParams(vmem_limit_bytes=8 << 20),
        cost_estimate=pl.CostEstimate(flops=flops, bytes_accessed=1 << 20, transcendentals=0),
        **kwargs,
    )


def dma(*shape):
    return pltpu.SemaphoreType.DMA(shape)


def pairs_sum(value, axis, size, steps):
    for step in steps:
        value = value + lax.ppermute(value, axis, [(i, i ^ step) for i in range(size)])
    return value


def scen_sum(value):
    others = [lax.ppermute(value, "scen", [(i, (i & 4) | ((i + k) & 3)) for i in range(8)]) for k in (1, 2, 3)]
    value = (value + others[0]) + (others[1] + others[2])
    return value + lax.ppermute(value, "scen", [(i, i ^ 4) for i in range(8)])


def swap(slab_count, send_chip, send_near):
    near = []
    for i in range(1, slab_count - 1, 2):
        near += [(i, i + 1), (i + 1, i)]
    got_near = lax.ppermute(send_near, "slab", near)
    got_chip = lax.ppermute(send_chip, "slab", [(i, i ^ 1) for i in range(slab_count)])
    return got_chip, got_near


def on_device(start, flow_east, flow_north, wells, monitors, control, multiplier, threshold):
    scen_count = lax.axis_size("scen")
    slab_count = lax.axis_size("slab")
    odd = lax.axis_index("slab") % 2
    in_hbm = functools.partial(pltpu.with_memory_space_constraint, memory_space=pltpu.HBM)
    half = (2, 4096)

    low, high = start[0, 0], start[0, NZ - 1]
    halos = swap(slab_count, jnp.where(odd == 0, high, low), jnp.where(odd == 0, low, high))
    consensus = scen_sum((control + multiplier)[0]) / scen_count

    c0, ve, vn, ahead = call(
        first_kernel, "step0", 3 << 30,
        in_specs=[HBM] * 3, out_specs=[VM] * 4, out_shape=[FIELD] * 4, scratch_shapes=[dma(NZ, 6)],
    )(in_hbm(start), in_hbm(flow_east), in_hbm(flow_north))
    c, send_chip, send_near, co = call(
        rate_kernel, "rate", 1 << 28,
        in_specs=[VM] * 5 + [HBM], out_specs=[VM] * 4, out_shape=[FIELD, PLANE, PLANE, FIELD],
        scratch_shapes=[pltpu.VMEM((NZ, NX, NY), jnp.int32), dma(NZ)],
        input_output_aliases={2: 0},
    )(*halos, ahead, c0, consensus, in_hbm(wells))
    states = [c0, c]
    for k in range(1, STEPS):
        halos = swap(slab_count, send_chip, send_near)
        ahead = call(step_kernel, f"step{k}", 3 << 30, in_specs=[VM] * 4, out_specs=VM, out_shape=FIELD)(c, ve, vn, co)
        if k < STEPS - 1:
            c, send_chip, send_near = call(
                fix_kernel, f"fix{k}", 1 << 26,
                in_specs=[VM] * 3, out_specs=[VM] * 3, out_shape=[FIELD, PLANE, PLANE],
                input_output_aliases={2: 0},
            )(*halos, ahead)
            states.append(c)
    final, adjoint, send_chip, send_near, sums, unused = call(
        seed_kernel, "seed", 1 << 28,
        in_specs=[VM] * 3 + [HBM], out_specs=[HBM] + [VM] * 5,
        out_shape=[jax.ShapeDtypeStruct((1, NZ, NX, NY), f32), FIELD, PLANE, PLANE, jax.ShapeDtypeStruct((16, 128), f32), FIELD],
        input_output_aliases={2: 5},
        scratch_shapes=[pltpu.VMEM((NZ, NX, NY), f32), pltpu.VMEM((NZ, NX, NY), jnp.int32), dma(NZ), pltpu.SemaphoreType.DMA],
    )(*halos, ahead, in_hbm(monitors))
    grads = ()
    rounds = [1, 2, 4, 8]
    for k in range(STEPS - 1, 0, -1):
        halos = swap(slab_count, send_chip, send_near)
        sums = pairs_sum(sums, "slab", slab_count, rounds[:1])
        rounds = rounds[1:]
        ahead, grad = call(
            adjoint_kernel, f"adjoint{k}", 4 << 30,
            in_specs=[VM] * (5 + len(grads)), out_specs=[VM] * 2, out_shape=[FIELD] * 2,
            input_output_aliases={5: 1} if grads else {},
        )(states[k], adjoint, ve, vn, co, *grads)
        sums, ahead, grad = lax.optimization_barrier((sums, ahead, grad))
        grads = (grad,)
        if k > 1:
            adjoint, send_chip, send_near = call(
                fix_kernel, f"back{k}", 1 << 26,
                in_specs=[VM] * 3, out_specs=[VM] * 3, out_shape=[FIELD, PLANE, PLANE],
                input_output_aliases={2: 0},
            )(*halos, ahead)
    coarse, unused = call(
        restrict_kernel, "restrict", 1 << 28,
        in_specs=[VM] * 5 + [HBM], out_specs=[VM] * 2, out_shape=[jax.ShapeDtypeStruct(half, f32), FIELD],
        input_output_aliases={2: 1},
        scratch_shapes=[pltpu.VMEM((2, NX, NY), f32), pltpu.VMEM((NZ, NX, NY), jnp.int32), dma(NZ)],
    )(*halos, ahead, c0, grad, in_hbm(wells))

    sums = pairs_sum(sums, "slab", slab_count, rounds)
    mass, count = sums[0:1], jnp.maximum(sums[8:9], 1.0)
    scaled = (mass / count - threshold[0]) / SOFT_WIDTH
    share = 1.0 / ((1.0 - BETA_LEVEL) * scen_count)
    weight = jax.nn.sigmoid(scaled) * share
    soft_term = SOFT_WIDTH * jax.nn.softplus(scaled) * share
    risk = scen_sum(soft_term)
    coarse_cells = NZ * slab_count * NX * NY / 64.0
    scale = (weight * 2.0 / count * (-TIME_STEP * coarse_cells))[0, 0]
    total = scen_sum(coarse * scale)
    consensus_next = consensus - total
    multiplier_next = multiplier + control - consensus_next[None]
    return (final, consensus_next, multiplier_next, threshold + risk[0, :1])


def solution(mesh):
    placed = (
        P("scen", "slab", None, None),
        P("scen", "slab", None, None),
        P("scen", "slab", None, None),
        P("slab", None, None),
        P("slab", None, None),
        P("scen", "slab", None),
        P("scen", "slab", None),
        P(),
    )
    return jax.shard_map(
        on_device,
        mesh=mesh,
        in_specs=placed,
        out_specs=(P("scen", "slab", None, None), P("slab", None), P("scen", "slab", None), P()),
        check_vma=False,
    )
```

```python
import functools

import jax
import jax.numpy as jnp
from jax import lax
from jax.experimental import pallas as pl
from jax.experimental.pallas import tpu as pltpu
from jax.sharding import PartitionSpec as P


STEPS = 4
EPS_LIMIT = 0.01
TIME_STEP = 0.25
DIFF_FLAT = 0.1
DIFF_VERTICAL = 0.25
BETA_LEVEL = 0.75
SOFT_WIDTH = 0.25

NZ, NX, NY = 8, 256, 256
HP = NX + 8
ZP = 2 * HP
F0 = 8
ROWS = F0 + NZ * ZP + 8
SEG = HP // 8
VERT = TIME_STEP * DIFF_VERTICAL
KEEP = 1.0 - 2.0 * VERT
f32 = jnp.float32
VM = pl.BlockSpec(memory_space=pltpu.VMEM)
HBM = pl.BlockSpec(memory_space=pltpu.HBM)
FIELD = jax.ShapeDtypeStruct((ROWS, 128), f32)
PLANE = jax.ShapeDtypeStruct((NX, NY), f32)


def seg_load(ref, z, h, r):
    return ref[pl.ds(F0 + z * ZP + h * HP + r, 8, stride=SEG), :]


def seg_store(ref, z, h, r, value):
    ref[pl.ds(F0 + z * ZP + h * HP + r, 8, stride=SEG), :] = value


def block_rows(z, h, j):
    return pl.ds(pl.multiple_of(F0 + z * ZP + h * HP + 8 * j, 8), 8)


def zero_plane_pads(ref, z):
    for h in range(2):
        ref[pl.ds(pl.multiple_of(F0 + z * ZP + h * HP + NX, 8), 8), :] = jnp.zeros((8, 128), f32)


def zero_pads(ref):
    zeros = jnp.zeros((8, 128), f32)
    ref[0:8, :] = zeros
    ref[ROWS - 8 : ROWS, :] = zeros
    for z in range(NZ):
        for h in range(2):
            start = F0 + z * ZP + h * HP + NX
            ref[start : start + 8, :] = zeros


def limiter(b, f, sb, sf):
    p = b * f
    q = p * p + EPS_LIMIT * EPS_LIMIT
    s = q * lax.rsqrt(q)
    r = lax.rsqrt(sb + sf + EPS_LIMIT)
    return ((p + s) * (r * r)) * ((b + f) + f)


def limiter_slopes(b, f, sb, sf):
    p = b * f
    q = p * p + EPS_LIMIT * EPS_LIMIT
    rs = lax.rsqrt(q)
    s = q * rs
    r = lax.rsqrt(sb + sf + EPS_LIMIT)
    r = r * r
    w = (p + s) * r
    u = (b + f) + f
    r2 = r + r
    slope_b = (f * rs - b * r2) * u + 1.0
    slope_f = (b * rs - f * r2) * u + 2.0
    return w, u, slope_b, slope_f


def lane_masks():
    lane = lax.broadcasted_iota(jnp.int32, (8, 128), 1)
    return lane == 0, lane == 127


def from_left(pair, first, edge):
    rolled = [pltpu.roll(v, 1, 1) for v in pair]
    return [jnp.where(edge, first, rolled[0]), jnp.where(edge, rolled[0], rolled[1])]


def from_right(pair, last, edge):
    rolled = [pltpu.roll(v, 127, 1) for v in pair]
    return [jnp.where(edge, rolled[1], rolled[0]), jnp.where(edge, last, rolled[1])]


def vertical_sum(ref, z, h, r):
    if isinstance(z, int) and z == 0:
        return seg_load(ref, 1, h, r)
    if isinstance(z, int) and z == NZ - 1:
        return seg_load(ref, NZ - 2, h, r)
    return seg_load(ref, z - 1, h, r) + seg_load(ref, z + 1, h, r)


def forward_plane(z, unroll, c_ref, ve_ref, vn_ref, co_ref, out_ref, slope_refs):
    at_first, at_last = lane_masks()

    def flux(v, c6, b, f, sb, sf, refs, h, r):
        if refs is None:
            corrected = v * (c6 + limiter(b, f, sb, sf))
        else:
            w, u, slope_b, slope_f = limiter_slopes(b, f, sb, sf)
            vw = v * w
            seg_store(refs[0], z, h, r, vw * slope_b)
            seg_store(refs[1], z, h, r, vw * slope_f - 6.0 * DIFF_FLAT)
            corrected = v * c6 + vw * u
        return corrected - (6.0 * DIFF_FLAT) * f

    def one(r, c, b, sb, before):
        after = [seg_load(c_ref, z, h, r + 1) for h in (0, 1)]
        left = from_left(c, 0.0, at_first)
        right = from_right(c, 0.0, at_last)
        f, sf, gx, gy = [], [], [], []
        for h in (0, 1):
            c6 = 6.0 * c[h]
            fx = after[h] - c[h]
            sx = fx * fx
            gx.append(flux(seg_load(ve_ref, z, h, r), c6, b[h], fx, sb[h], sx, slope_refs and slope_refs[:2], h, r))
            by = c[h] - left[h]
            fy = right[h] - c[h]
            gy.append(flux(seg_load(vn_ref, z, h, r), c6, by, fy, by * by, fy * fy, slope_refs and slope_refs[2:], h, r))
            f.append(fx)
            sf.append(sx)
        gl = from_left(gy, (-6.0 * DIFF_FLAT) * c[0], at_first)
        for h in (0, 1):
            vertical = VERT * vertical_sum(c_ref, z, h, r)
            keep = KEEP if co_ref is None else seg_load(co_ref, z, h, r)
            flow = (gx[h] - before[h]) + (gy[h] - gl[h])
            seg_store(out_ref, z, h, r, keep * c[h] + vertical - (TIME_STEP / 6.0) * flow)
        return after, f, sf, gx

    c, b, sb, before = [], [], [], []
    for h in (0, 1):
        m2 = seg_load(c_ref, z, h, -2)
        m1 = seg_load(c_ref, z, h, -1)
        c0 = seg_load(c_ref, z, h, 0)
        bm = m1 - m2
        fm = c0 - m1
        sm = fm * fm
        before.append(flux(seg_load(ve_ref, z, h, -1), 6.0 * m1, bm, fm, bm * bm, sm, None, h, -1))
        c.append(c0)
        b.append(fm)
        sb.append(sm)

    def block(i, carry):
        for j in range(unroll):
            carry = one(i * unroll + j, *carry)
        return carry

    lax.fori_loop(0, SEG // unroll, block, (c, b, sb, before))
    zero_plane_pads(out_ref, z)


def over_planes(plane):
    plane(0)

    def inner(z, unused):
        plane(z)
        return unused

    lax.fori_loop(1, NZ - 1, inner, 0)
    plane(NZ - 1)


def first_kernel(start_ref, east_ref, north_ref, c_ref, ve_ref, vn_ref, out_ref, sem):
    def copies(z):
        made = []
        for source, target in ((start_ref, c_ref), (east_ref, ve_ref), (north_ref, vn_ref)):
            for h in (0, 1):
                made.append(
                    pltpu.make_async_copy(
                        source.at[0, z, :, pl.ds(h * 128, 128)],
                        target.at[pl.ds(pl.multiple_of(F0 + z * ZP + h * HP, 8), NX), :],
                        sem.at[z, len(made)],
                    )
                )
        return made

    ahead = 3
    for z in range(ahead):
        for copy in copies(z):
            copy.start()
    for ref in (c_ref, ve_ref, vn_ref, out_ref):
        zero_pads(ref)
    for copy in copies(0):
        copy.wait()

    def plane(z):
        if isinstance(z, int) and z == NZ - 1:
            pass
        else:
            for copy in copies(z + 1):
                copy.wait()

            @pl.when(z + ahead < NZ)
            def _():
                for copy in copies(z + ahead):
                    copy.start()

        forward_plane(z, 11, c_ref, ve_ref, vn_ref, None, out_ref, None)

    over_planes(plane)


def step_kernel(c_ref, ve_ref, vn_ref, co_ref, out_ref, *slope_refs):
    zero_pads(out_ref)
    for i, ref in enumerate(slope_refs):
        ref[0:F0, :] = jnp.full((F0, 128), -6.0 * DIFF_FLAT if i % 2 else 0.0, f32)
    over_planes(lambda z: forward_plane(z, 11, c_ref, ve_ref, vn_ref, co_ref, out_ref, slope_refs))


def facing():
    z_chip = jnp.where(lax.axis_index("slab") % 2 == 0, NZ - 1, 0)
    return z_chip, NZ - 1 - z_chip


def fix_planes(chip_ref, near_ref, field_ref, target_ref, send_chip_ref=None, send_near_ref=None, prior_ref=None):
    z_chip, z_near = facing()
    slab = lax.axis_index("slab")
    near_share = jnp.where((slab > 0) & (slab < lax.axis_size("slab") - 1), VERT, 0.0)

    def block(j, unused):
        for h in (0, 1):
            lanes = slice(h * 128, h * 128 + 128)
            rows = pl.ds(pl.multiple_of(8 * j, 8), 8)
            for z, halo_ref, send_ref, share in (
                (z_chip, chip_ref, send_chip_ref, VERT),
                (z_near, near_ref, send_near_ref, near_share),
            ):
                at = block_rows(z, h, j)
                halo = halo_ref[rows, lanes]
                if prior_ref is not None:
                    halo = halo + share * prior_ref[at, :]
                value = field_ref[at, :] + VERT * halo
                target_ref[at, :] = value
                if send_ref is not None:
                    send_ref[rows, lanes] = value
        return unused

    lax.fori_loop(0, NX // 8, block, 0, unroll=4)


def fix_kernel(chip_ref, near_ref, field_ref, out_ref, send_chip_ref, send_near_ref):
    fix_planes(chip_ref, near_ref, field_ref, out_ref, send_chip_ref, send_near_ref)


def send_planes(field_ref, send_chip_ref, send_near_ref):
    z_chip, z_near = facing()

    def block(j, unused):
        for h in (0, 1):
            lanes = slice(h * 128, h * 128 + 128)
            rows = pl.ds(pl.multiple_of(8 * j, 8), 8)
            send_chip_ref[rows, lanes] = field_ref[block_rows(z_chip, h, j), :]
            send_near_ref[rows, lanes] = field_ref[block_rows(z_near, h, j), :]
        return unused

    lax.fori_loop(0, NX // 8, block, 0, unroll=4)


def rate_kernel(chip_ref, near_ref, field_ref, c0_ref, cons_ref, wells_ref, out_ref, send_chip_ref, send_near_ref, co_ref, wide_ref):
    lane = lax.broadcasted_iota(jnp.int32, (8, 128), 1)
    sub = lax.broadcasted_iota(jnp.int32, (8, 128), 0)
    base = jnp.where(sub < 4, 0, 64) + lane // 4
    zero_pads(co_ref)

    def prolong(j, unused):
        for p in (0, 1):
            coarse = cons_ref[pl.ds(p, 1), pl.ds(pl.multiple_of(j * 128, 128), 128)]
            coarse = jnp.broadcast_to(coarse * TIME_STEP, (8, 128))
            for h in (0, 1):
                wide_ref[p, pl.ds(pl.multiple_of(8 * j, 8), 8), h * 128 : h * 128 + 128] = jnp.take_along_axis(
                    coarse, base + 32 * h, axis=1
                )
        return unused

    lax.fori_loop(0, NX // 8, prolong, 0, unroll=8)

    def block(j, unused):
        rows = pl.ds(pl.multiple_of(8 * j, 8), 8)
        for h in (0, 1):
            lanes = slice(h * 128, h * 128 + 128)
            for p in (0, 1):
                wide = wide_ref[p, rows, lanes]
                for z in range(4 * p, 4 * p + 4):
                    rate = wells_ref[z, rows, lanes].astype(f32) * wide
                    at = block_rows(z, h, j)
                    co_ref[at, :] = KEEP - rate
                    out_ref[at, :] = field_ref[at, :] - rate * c0_ref[at, :]
        return unused

    lax.fori_loop(0, NX // 8, block, 0, unroll=2)
    fix_planes(chip_ref, near_ref, out_ref, out_ref, send_chip_ref, send_near_ref)


def seed_kernel(chip_ref, near_ref, ahead_ref, monitors_ref, final_ref, adjoint_ref, send_chip_ref, send_near_ref, field_ref):
    zero_pads(adjoint_ref)
    fix_planes(chip_ref, near_ref, ahead_ref, field_ref)

    def block(j, sums):
        mass, count = sums
        rows = pl.ds(pl.multiple_of(8 * j, 8), 8)
        for z in range(NZ):
            for h in (0, 1):
                lanes = slice(h * 128, h * 128 + 128)
                value = field_ref[block_rows(z, h, j), :]
                final_ref[0, z, rows, lanes] = value
                monitor = monitors_ref[z, rows, lanes].astype(f32)
                seed = monitor * value
                adjoint_ref[block_rows(z, h, j), :] = seed
                mass[z % 4] = mass[z % 4] + seed * value
                count[z % 4] = count[z % 4] + monitor
        return mass, count

    zeros = [jnp.zeros((8, 128), f32)] * 4
    mass, count = lax.fori_loop(0, NX // 8, block, (list(zeros), list(zeros)))
    for part, start in ((mass, 0), (count, 128)):
        part = (part[0] + part[1]) + (part[2] + part[3])
        part = jnp.sum(jnp.sum(part, axis=0, keepdims=True), axis=1, keepdims=True)
        send_chip_ref[NX : NX + 8, start : start + 128] = jnp.broadcast_to(part, (8, 128))
    send_planes(adjoint_ref, send_chip_ref, send_near_ref)


def adjoint_plane(z, unroll, fields, rg_in_ref, out_ref, rg_ref):
    a_ref, c_ref, ve_ref, vn_ref, co_ref, xb_ref, xf_ref, yb_ref, yf_ref = fields
    at_first, at_last = lane_masks()

    def one(r, a, next_a, vg, behind, front):
        far_a = [seg_load(a_ref, z, h, r + 2) for h in (0, 1)]
        right = from_right(a, 0.0, at_last)
        vy, back_y, front_y = [], [], []
        for h in (0, 1):
            g = right[h] - a[h]
            vy.append(seg_load(vn_ref, z, h, r) * g)
            back_y.append(seg_load(yb_ref, z, h, r) * g)
            front_y.append(seg_load(yf_ref, z, h, r) * g)
        fl = from_left(front_y, (-6.0 * DIFF_FLAT) * a[0], at_first)
        kr = from_right(back_y, 0.0, at_last)
        new_vg, new_behind, new_front = [], [], []
        for h in (0, 1):
            g = far_a[h] - next_a[h]
            ahead = seg_load(xb_ref, z, h, r + 1) * g + front[h]
            new_vg.append(seg_load(ve_ref, z, h, r + 1) * g)
            new_front.append(seg_load(xf_ref, z, h, r + 1) * g)
            new_behind.append(ahead)
            here = ((back_y[h] - front_y[h]) + (fl[h] - kr[h])) + (behind[h] - ahead) + 6.0 * (vg[h] + vy[h])
            vertical = VERT * vertical_sum(a_ref, z, h, r)
            out = seg_load(co_ref, z, h, r) * a[h] + vertical + (TIME_STEP / 6.0) * here
            seg_store(out_ref, z, h, r, out)
            grad = seg_load(c_ref, z, h, r) * a[h]
            if rg_in_ref is not None:
                grad = grad + seg_load(rg_in_ref, z, h, r)
            seg_store(rg_ref, z, h, r, grad)
        return next_a, far_a, new_vg, new_behind, new_front

    a, next_a, vg, behind, front = [], [], [], [], []
    for h in (0, 1):
        am = seg_load(a_ref, z, h, -1)
        a0 = seg_load(a_ref, z, h, 0)
        a1 = seg_load(a_ref, z, h, 1)
        gm = a0 - am
        g0 = a1 - a0
        a.append(a0)
        next_a.append(a1)
        vg.append(seg_load(ve_ref, z, h, 0) * g0)
        behind.append(seg_load(xb_ref, z, h, 0) * g0 + seg_load(xf_ref, z, h, -1) * gm)
        front.append(seg_load(xf_ref, z, h, 0) * g0)

    def block(i, carry):
        for j in range(unroll):
            carry = one(i * unroll + j, *carry)
        return carry

    lax.fori_loop(0, SEG // unroll, block, (a, next_a, vg, behind, front))
    zero_plane_pads(out_ref, z)


def edge_planes(fields, rg_in_ref, out_ref, rg_ref, send_chip_ref, send_near_ref):
    zero_pads(out_ref)
    for z in (0, NZ - 1):
        adjoint_plane(z, 11, fields, rg_in_ref, out_ref, rg_ref)
    send_planes(out_ref, send_chip_ref, send_near_ref)


def edge_kernel(*refs):
    edge_planes(refs[:9], None, *refs[9:])


def turn_kernel(chip_ref, near_ref, ahead_ref, *refs):
    rest, rg_in_ref, (a_ref, out_ref, rg_ref, send_chip_ref, send_near_ref) = refs[:8], refs[8], refs[9:]
    fix_planes(chip_ref, near_ref, ahead_ref, a_ref)
    edge_planes((a_ref,) + rest, rg_in_ref, out_ref, rg_ref, send_chip_ref, send_near_ref)


def inner_kernel(has_grad, *refs):
    fields, (out_in_ref, rg_in_ref, out_ref, rg_ref) = refs[:9], refs[9:]

    def inner(z, unused):
        adjoint_plane(z, 11, fields, rg_in_ref if has_grad else None, out_ref, rg_ref)
        return unused

    lax.fori_loop(1, NZ - 1, inner, 0)


def last_kernel(chip_ref, near_ref, prior_ref, ahead_ref, *refs):
    rest, rg_in_ref, (a_ref, out_ref, rg_ref) = refs[:8], refs[8], refs[9:]
    fix_planes(chip_ref, near_ref, ahead_ref, a_ref, prior_ref=prior_ref)
    zero_pads(out_ref)
    over_planes(lambda z: adjoint_plane(z, 11, (a_ref,) + rest, rg_in_ref, out_ref, rg_ref))


def restrict_kernel(share, cells, limit_ref, chip_ref, near_ref, prior_ref, ahead_ref, c0_ref, rg_ref, wells_ref, sums_ref, out_ref, field_ref, wide_ref):
    fix_planes(chip_ref, near_ref, ahead_ref, field_ref, prior_ref=prior_ref)
    count = jnp.maximum(sums_ref[0:8, 128:256], 1.0)
    scaled = (sums_ref[0:8, 0:128] / count - limit_ref[0]) / SOFT_WIDTH
    small = jnp.exp(-jnp.abs(scaled))
    weight = jnp.where(scaled >= 0.0, 1.0, small) / (1.0 + small) * share
    soft = SOFT_WIDTH * (jnp.maximum(scaled, 0.0) + jnp.log1p(small)) * share
    out_ref[0:2, NX * 16 : NX * 16 + 128] = soft[0:2, :]
    scale = weight * 2.0 / count * (-TIME_STEP * cells)

    def block(j, unused):
        rows = pl.ds(pl.multiple_of(8 * j, 8), 8)
        for h in (0, 1):
            lanes = slice(h * 128, h * 128 + 128)
            for p in (0, 1):
                parts = []
                for z in range(4 * p, 4 * p + 4):
                    at = block_rows(z, h, j)
                    parts.append(wells_ref[z, rows, lanes].astype(f32) * (rg_ref[at, :] + c0_ref[at, :] * field_ref[at, :]))
                wide_ref[p, rows, lanes] = ((parts[0] + parts[1]) + (parts[2] + parts[3])) * scale
        return unused

    lax.fori_loop(0, NX // 8, block, 0, unroll=2)
    fine = lax.broadcasted_iota(jnp.int32, (NY, 128), 0) // 4
    coarse = lax.broadcasted_iota(jnp.int32, (NY, 128), 1) % 64
    sums = jnp.where(fine == coarse, 1.0, 0.0).astype(f32)
    row = lax.broadcasted_iota(jnp.int32, (NX, 128), 0) % 8
    lane = lax.broadcasted_iota(jnp.int32, (NX, 128), 1)
    own = (row < 4) == (lane < 64)
    for p in (0, 1):
        part = jnp.dot(wide_ref[p], sums, precision=lax.Precision.HIGHEST, preferred_element_type=f32)
        part = jnp.where(own, part, 0.0).reshape(NX // 8, 8, 128).sum(axis=1)
        for j in range(NX // 8):
            out_ref[p : p + 1, j * 128 : (j + 1) * 128] = part[j : j + 1, :]


def call(kernel, flops, **kwargs):
    return pl.pallas_call(
        kernel,
        compiler_params=pltpu.CompilerParams(vmem_limit_bytes=8 << 20),
        cost_estimate=pl.CostEstimate(flops=flops, bytes_accessed=1 << 20, transcendentals=0),
        **kwargs,
    )


def dma(*shape):
    return pltpu.SemaphoreType.DMA(shape)


def pair_sum(value, axis, size, step):
    return value + lax.ppermute(value, axis, [(i, i ^ step) for i in range(size)])


def scen_sum(value):
    others = [lax.ppermute(value, "scen", [(i, (i & 4) | ((i + k) & 3)) for i in range(8)]) for k in (1, 2, 3)]
    value = (value + others[0]) + (others[1] + others[2])
    return pair_sum(value, "scen", 8, 4)


def swap(slab_count, send_chip, send_near):
    near = []
    for i in range(1, slab_count - 1, 2):
        near += [(i, i + 1), (i + 1, i)]
    got_near = lax.ppermute(send_near, "slab", near)
    got_chip = lax.ppermute(send_chip, "slab", [(i, i ^ 1) for i in range(slab_count)])
    return got_chip, got_near


def on_device(start, flow_east, flow_north, wells, monitors, control, multiplier, threshold):
    scen_count = lax.axis_size("scen")
    slab_count = lax.axis_size("slab")
    odd = lax.axis_index("slab") % 2
    in_hbm = functools.partial(pltpu.with_memory_space_constraint, memory_space=pltpu.HBM)

    low, high = start[0, 0], start[0, NZ - 1]
    halos = swap(slab_count, jnp.where(odd == 0, high, low), jnp.where(odd == 0, low, high))
    consensus = scen_sum((control + multiplier)[0]) / scen_count

    c0, ve, vn, ahead = call(
        first_kernel, 3 << 30,
        in_specs=[HBM] * 3, out_specs=[VM] * 4, out_shape=[FIELD] * 4, scratch_shapes=[dma(NZ, 6)],
    )(in_hbm(start), in_hbm(flow_east), in_hbm(flow_north))
    c, send_chip, send_near, co = call(
        rate_kernel, 1 << 28,
        in_specs=[VM] * 6, out_specs=[VM] * 4, out_shape=[FIELD, PLANE, PLANE, FIELD],
        scratch_shapes=[pltpu.VMEM((2, NX, NY), f32)],
        input_output_aliases={2: 0},
    )(*halos, ahead, c0, consensus, wells)
    states = [c0, c]
    slopes = [()]
    for k in range(1, STEPS):
        halos = swap(slab_count, send_chip, send_near)
        ahead, *made = call(step_kernel, 3 << 30, in_specs=[VM] * 4, out_specs=[VM] * 5, out_shape=[FIELD] * 5)(c, ve, vn, co)
        slopes.append(tuple(made))
        if k < STEPS - 1:
            c, send_chip, send_near = call(
                fix_kernel, 1 << 26,
                in_specs=[VM] * 3, out_specs=[VM] * 3, out_shape=[FIELD, PLANE, PLANE],
                input_output_aliases={2: 0},
            )(*halos, ahead)
            states.append(c)
    final, seed, send_chip, send_near, _ = call(
        seed_kernel, 1 << 28,
        in_specs=[VM] * 4, out_specs=[VM] * 5,
        out_shape=[
            jax.ShapeDtypeStruct((1, NZ, NX, NY), f32), FIELD, jax.ShapeDtypeStruct((NX + 8, NY), f32), PLANE, FIELD,
        ],
        input_output_aliases={2: 4},
    )(*halos, ahead, monitors)

    def rest(k):
        return (states[k], ve, vn, co) + slopes[k]

    def inner(k, adjoint, ahead, grad):
        return call(
            functools.partial(inner_kernel, k < STEPS - 1), 2 << 30,
            in_specs=[VM] * 11, out_specs=[VM] * 2, out_shape=[FIELD] * 2, input_output_aliases={9: 0, 10: 1},
        )(adjoint, *rest(k), ahead, grad)

    halos4 = swap(slab_count, send_chip, send_near)
    ahead, grad, send_chip5, send_near5 = call(
        edge_kernel, 1 << 30,
        in_specs=[VM] * 9, out_specs=[VM] * 4, out_shape=[FIELD, FIELD, PLANE, PLANE],
    )(seed, *rest(3))
    halos5 = swap(slab_count, send_chip5, send_near5)
    sums = send_chip[NX:] + halos4[0][NX:]
    sums = pair_sum(sums, "slab", slab_count, 2)
    ahead, grad = inner(3, seed, ahead, grad)
    adjoint3, ahead, grad, send_chip, send_near = call(
        turn_kernel, 1 << 30,
        in_specs=[VM] * 12, out_specs=[VM] * 5, out_shape=[FIELD, FIELD, FIELD, PLANE, PLANE],
        input_output_aliases={2: 0, 11: 2},
    )(*halos4, ahead, *rest(2), grad)
    halos6 = swap(slab_count, send_chip, send_near)
    sums = pair_sum(sums, "slab", slab_count, 4)
    ahead, grad = inner(2, adjoint3, ahead, grad)
    sums = pair_sum(sums, "slab", slab_count, 8)
    _, ahead, grad = call(
        last_kernel, 3 << 30,
        in_specs=[VM] * 13, out_specs=[VM] * 3, out_shape=[FIELD] * 3, input_output_aliases={3: 0, 12: 2},
    )(*halos5, seed, ahead, *rest(1), grad)
    share = 1.0 / ((1.0 - BETA_LEVEL) * scen_count)
    coarse_cells = NZ * slab_count * NX * NY / 64.0
    coarse, _ = call(
        functools.partial(restrict_kernel, share, coarse_cells), 1 << 28,
        in_specs=[pl.BlockSpec(memory_space=pltpu.SMEM)] + [VM] * 8, out_specs=[VM] * 2,
        out_shape=[jax.ShapeDtypeStruct((2, 4096 + 128), f32), FIELD],
        scratch_shapes=[pltpu.VMEM((2, NX, NY), f32)],
        input_output_aliases={4: 1},
    )(threshold, *halos6, adjoint3, ahead, c0, grad, wells, sums)
    total = scen_sum(coarse)
    consensus_next = consensus - total[:, :4096]
    multiplier_next = multiplier + control - consensus_next[None]
    return (final, consensus_next, multiplier_next, threshold + total[0, 4096:4097])


def solution(mesh):
    placed = (
        P("scen", "slab", None, None),
        P("scen", "slab", None, None),
        P("scen", "slab", None, None),
        P("slab", None, None),
        P("slab", None, None),
        P("scen", "slab", None),
        P("scen", "slab", None),
        P(),
    )
    return jax.shard_map(
        on_device,
        mesh=mesh,
        in_specs=placed,
        out_specs=(P("scen", "slab", None, None), P("slab", None), P("scen", "slab", None), P()),
        check_vma=False,
    )
```

```python
import functools

import jax
import jax.numpy as jnp
from jax import lax
from jax.experimental import pallas as pl
from jax.experimental.pallas import tpu as pltpu
from jax.sharding import PartitionSpec as P


STEPS = 4
EPS_LIMIT = 0.01
TIME_STEP = 0.25
DIFF_FLAT = 0.1
DIFF_VERTICAL = 0.25
BETA_LEVEL = 0.75
SOFT_WIDTH = 0.25

NZ, NX, NY = 8, 256, 256
HP = NX + 8
ZP = 2 * HP
F0 = 8
ROWS = F0 + NZ * ZP + 8
SEG = HP // 8
UNROLL = 11
VERT = TIME_STEP * DIFF_VERTICAL
KEEP = 1.0 - 2.0 * VERT
f32 = jnp.float32
VM = pl.BlockSpec(memory_space=pltpu.VMEM)
HBM = pl.BlockSpec(memory_space=pltpu.HBM)
FIELD = jax.ShapeDtypeStruct((ROWS, 128), f32)
PLANE = jax.ShapeDtypeStruct((NX, NY), f32)


def seg_load(ref, z, h, r):
    return ref[pl.ds(F0 + z * ZP + h * HP + r, 8, stride=SEG), :]


def seg_store(ref, z, h, r, value):
    ref[pl.ds(F0 + z * ZP + h * HP + r, 8, stride=SEG), :] = value


def block_rows(z, h, j):
    return pl.ds(pl.multiple_of(F0 + z * ZP + h * HP + 8 * j, 8), 8)


def zero_plane_pads(ref, z):
    for h in range(2):
        ref[pl.ds(pl.multiple_of(F0 + z * ZP + h * HP + NX, 8), 8), :] = jnp.zeros((8, 128), f32)


def zero_pads(ref):
    zeros = jnp.zeros((8, 128), f32)
    ref[0:8, :] = zeros
    ref[ROWS - 8 : ROWS, :] = zeros
    for z in range(NZ):
        for h in range(2):
            start = F0 + z * ZP + h * HP + NX
            ref[start : start + 8, :] = zeros


def limiter(b, f, sb, sf):
    p = b * f
    q = p * p + EPS_LIMIT * EPS_LIMIT
    s = q * lax.rsqrt(q)
    r = lax.rsqrt(sb + sf + EPS_LIMIT)
    return ((p + s) * (r * r)) * ((b + f) + f)


def limiter_slopes(b, f, sb, sf):
    p = b * f
    q = p * p + EPS_LIMIT * EPS_LIMIT
    rs = lax.rsqrt(q)
    s = q * rs
    r = lax.rsqrt(sb + sf + EPS_LIMIT)
    r = r * r
    w = (p + s) * r
    u = (b + f) + f
    r2 = r + r
    slope_b = (f * rs - b * r2) * u + 1.0
    slope_f = (b * rs - f * r2) * u + 2.0
    return w, u, slope_b, slope_f


def lane_masks():
    lane = lax.broadcasted_iota(jnp.int32, (8, 128), 1)
    return lane == 0, lane == 127


def from_left(pair, first, edge):
    rolled = [pltpu.roll(v, 1, 1) for v in pair]
    return [jnp.where(edge, first, rolled[0]), jnp.where(edge, rolled[0], rolled[1])]


def from_right(pair, last, edge):
    rolled = [pltpu.roll(v, 127, 1) for v in pair]
    return [jnp.where(edge, rolled[1], rolled[0]), jnp.where(edge, last, rolled[1])]


def vertical_sum(ref, z, h, r):
    if isinstance(z, int) and z == 0:
        return seg_load(ref, 1, h, r)
    if isinstance(z, int) and z == NZ - 1:
        return seg_load(ref, NZ - 2, h, r)
    return seg_load(ref, z - 1, h, r) + seg_load(ref, z + 1, h, r)


def stage_rolls(stage_ref, ref, z, r, j, both):
    at_first, at_last = lane_masks()
    pair = [seg_load(ref, z, h, r) for h in (0, 1)]
    made = from_right(pair, 0.0, at_last) + (from_left(pair, 0.0, at_first) if both else [])
    for n, value in enumerate(made):
        start = (j * len(made) + n) * 8
        stage_ref[start : start + 8, :] = value


def staged(stage_ref, j, both):
    count = 4 if both else 2
    made = [stage_ref[(j * count + n) * 8 : (j * count + n) * 8 + 8, :] for n in range(count)]
    return made[:2], made[2:]


def next_block(z, next_z, i, unroll):
    last = i == SEG // unroll - 1
    return jnp.where(last, next_z, z), jnp.where(last, 0, (i + 1) * unroll)


def forward_plane(z, next_z, unroll, stage_ref, c_ref, ve_ref, vn_ref, co_ref, out_ref, slope_refs):
    at_first, _ = lane_masks()

    def flux(v, c6, b, f, sb, sf, refs, h, r):
        if refs is None:
            corrected = v * (c6 + limiter(b, f, sb, sf))
        else:
            w, u, slope_b, slope_f = limiter_slopes(b, f, sb, sf)
            vw = v * w
            seg_store(refs[0], z, h, r, vw * slope_b)
            seg_store(refs[1], z, h, r, vw * slope_f - 6.0 * DIFF_FLAT)
            corrected = v * c6 + vw * u
        return corrected - (6.0 * DIFF_FLAT) * f

    def one(r, j, following, c, b, sb, before):
        after = [seg_load(c_ref, z, h, r + 1) for h in (0, 1)]
        right, left = staged(stage_ref, j, True)
        stage_rolls(stage_ref, c_ref, following[0], following[1] + j, j, True)
        f, sf, gx, gy = [], [], [], []
        for h in (0, 1):
            c6 = 6.0 * c[h]
            fx = after[h] - c[h]
            sx = fx * fx
            gx.append(flux(seg_load(ve_ref, z, h, r), c6, b[h], fx, sb[h], sx, slope_refs and slope_refs[:2], h, r))
            by = c[h] - left[h]
            fy = right[h] - c[h]
            gy.append(flux(seg_load(vn_ref, z, h, r), c6, by, fy, by * by, fy * fy, slope_refs and slope_refs[2:], h, r))
            f.append(fx)
            sf.append(sx)
        gl = from_left(gy, (-6.0 * DIFF_FLAT) * c[0], at_first)
        for h in (0, 1):
            vertical = VERT * vertical_sum(c_ref, z, h, r)
            keep = KEEP if co_ref is None else seg_load(co_ref, z, h, r)
            flow = (gx[h] - before[h]) + (gy[h] - gl[h])
            seg_store(out_ref, z, h, r, keep * c[h] + vertical - (TIME_STEP / 6.0) * flow)
        return after, f, sf, gx

    c, b, sb, before = [], [], [], []
    for h in (0, 1):
        m2 = seg_load(c_ref, z, h, -2)
        m1 = seg_load(c_ref, z, h, -1)
        c0 = seg_load(c_ref, z, h, 0)
        bm = m1 - m2
        fm = c0 - m1
        sm = fm * fm
        before.append(flux(seg_load(ve_ref, z, h, -1), 6.0 * m1, bm, fm, bm * bm, sm, None, h, -1))
        c.append(c0)
        b.append(fm)
        sb.append(sm)

    def block(i, carry):
        following = next_block(z, next_z, i, unroll)
        for j in range(unroll):
            carry = one(i * unroll + j, j, following, *carry)
        return carry

    lax.fori_loop(0, SEG // unroll, block, (c, b, sb, before))
    zero_plane_pads(out_ref, z)


def stage_first(stage_ref, ref, z, unroll, both):
    for j in range(unroll):
        stage_rolls(stage_ref, ref, z, j, j, both)


def over_planes(plane):
    plane(0, 1)

    def inner(z, unused):
        plane(z, z + 1)
        return unused

    lax.fori_loop(1, NZ - 1, inner, 0)
    plane(NZ - 1, NZ - 1)


def first_kernel(start_ref, east_ref, north_ref, c_ref, ve_ref, vn_ref, out_ref, stage_ref, sem):
    def copies(z):
        made = []
        for source, target in ((start_ref, c_ref), (east_ref, ve_ref), (north_ref, vn_ref)):
            for h in (0, 1):
                made.append(
                    pltpu.make_async_copy(
                        source.at[0, z, :, pl.ds(h * 128, 128)],
                        target.at[pl.ds(pl.multiple_of(F0 + z * ZP + h * HP, 8), NX), :],
                        sem.at[z, len(made)],
                    )
                )
        return made

    ahead = 3
    for z in range(ahead):
        for copy in copies(z):
            copy.start()
    for ref in (c_ref, ve_ref, vn_ref, out_ref):
        zero_pads(ref)
    for copy in copies(0):
        copy.wait()
    stage_first(stage_ref, c_ref, 0, UNROLL, True)

    def plane(z, next_z):
        if isinstance(z, int) and z == NZ - 1:
            pass
        else:
            for copy in copies(z + 1):
                copy.wait()

            @pl.when(z + ahead < NZ)
            def _():
                for copy in copies(z + ahead):
                    copy.start()

        forward_plane(z, next_z, UNROLL, stage_ref, c_ref, ve_ref, vn_ref, None, out_ref, None)

    over_planes(plane)


def step_kernel(c_ref, ve_ref, vn_ref, co_ref, out_ref, *rest):
    slope_refs, stage_ref = rest[:4], rest[4]
    zero_pads(out_ref)
    stage_first(stage_ref, c_ref, 0, UNROLL, True)
    for i, ref in enumerate(slope_refs):
        ref[0:F0, :] = jnp.full((F0, 128), -6.0 * DIFF_FLAT if i % 2 else 0.0, f32)
    over_planes(
        lambda z, next_z: forward_plane(z, next_z, UNROLL, stage_ref, c_ref, ve_ref, vn_ref, co_ref, out_ref, slope_refs)
    )


def facing():
    z_chip = jnp.where(lax.axis_index("slab") % 2 == 0, NZ - 1, 0)
    return z_chip, NZ - 1 - z_chip


def fix_planes(chip_ref, near_ref, field_ref, target_ref, send_chip_ref=None, send_near_ref=None, prior_ref=None):
    z_chip, z_near = facing()
    slab = lax.axis_index("slab")
    near_share = jnp.where((slab > 0) & (slab < lax.axis_size("slab") - 1), VERT, 0.0)

    sides = ((z_chip, chip_ref, send_chip_ref, VERT), (z_near, near_ref, send_near_ref, near_share))

    def block(j, unused):
        rows = pl.ds(pl.multiple_of(8 * j, 8), 8)
        made = []
        for h in (0, 1):
            lanes = slice(h * 128, h * 128 + 128)
            for z, halo_ref, send_ref, share in sides:
                at = block_rows(z, h, j)
                halo = halo_ref[rows, lanes]
                if prior_ref is not None:
                    halo = halo + share * prior_ref[at, :]
                made.append((at, lanes, send_ref, field_ref[at, :] + VERT * halo))
        for at, lanes, send_ref, value in made:
            target_ref[at, :] = value
            if send_ref is not None:
                send_ref[rows, lanes] = value
        return unused

    lax.fori_loop(0, NX // 8, block, 0, unroll=4)


def fix_kernel(chip_ref, near_ref, field_ref, out_ref, send_chip_ref, send_near_ref):
    fix_planes(chip_ref, near_ref, field_ref, out_ref, send_chip_ref, send_near_ref)


def send_planes(field_ref, send_chip_ref, send_near_ref):
    z_chip, z_near = facing()

    def block(j, unused):
        rows = pl.ds(pl.multiple_of(8 * j, 8), 8)
        made = []
        for h in (0, 1):
            lanes = slice(h * 128, h * 128 + 128)
            made.append((send_chip_ref, lanes, field_ref[block_rows(z_chip, h, j), :]))
            made.append((send_near_ref, lanes, field_ref[block_rows(z_near, h, j), :]))
        for send_ref, lanes, value in made:
            send_ref[rows, lanes] = value
        return unused

    lax.fori_loop(0, NX // 8, block, 0, unroll=4)


def rate_kernel(chip_ref, near_ref, field_ref, c0_ref, cons_ref, wells_ref, out_ref, send_chip_ref, send_near_ref, co_ref, wide_ref):
    lane = lax.broadcasted_iota(jnp.int32, (8, 128), 1)
    sub = lax.broadcasted_iota(jnp.int32, (8, 128), 0)
    base = jnp.where(sub < 4, 0, 64) + lane // 4
    zero_pads(co_ref)

    def prolong(j, unused):
        for p in (0, 1):
            coarse = cons_ref[pl.ds(p, 1), pl.ds(pl.multiple_of(j * 128, 128), 128)]
            coarse = jnp.broadcast_to(coarse * TIME_STEP, (8, 128))
            for h in (0, 1):
                wide_ref[p, pl.ds(pl.multiple_of(8 * j, 8), 8), h * 128 : h * 128 + 128] = jnp.take_along_axis(
                    coarse, base + 32 * h, axis=1
                )
        return unused

    lax.fori_loop(0, NX // 8, prolong, 0, unroll=8)

    def block(j, unused):
        rows = pl.ds(pl.multiple_of(8 * j, 8), 8)
        for h in (0, 1):
            lanes = slice(h * 128, h * 128 + 128)
            rates = [wells_ref[z, rows, lanes].astype(f32) * wide_ref[z // 4, rows, lanes] for z in range(NZ)]
            values = [
                field_ref[block_rows(z, h, j), :] - rates[z] * c0_ref[block_rows(z, h, j), :] for z in range(NZ)
            ]
            for z in range(NZ):
                co_ref[block_rows(z, h, j), :] = KEEP - rates[z]
                out_ref[block_rows(z, h, j), :] = values[z]
        return unused

    lax.fori_loop(0, NX // 8, block, 0, unroll=2)
    fix_planes(chip_ref, near_ref, out_ref, out_ref, send_chip_ref, send_near_ref)


def seed_kernel(chip_ref, near_ref, ahead_ref, monitors_ref, adjoint_ref, send_chip_ref, send_near_ref, field_ref):
    zero_pads(adjoint_ref)
    fix_planes(chip_ref, near_ref, ahead_ref, field_ref)

    def block(j, sums):
        mass, count = sums
        rows = pl.ds(pl.multiple_of(8 * j, 8), 8)
        made = []
        for h in (0, 1):
            lanes = slice(h * 128, h * 128 + 128)
            for z in range(NZ):
                value = field_ref[block_rows(z, h, j), :]
                monitor = monitors_ref[z, rows, lanes].astype(f32)
                seed = monitor * value
                made.append((block_rows(z, h, j), seed))
                mass[z % 4] = mass[z % 4] + seed * value
                count[z % 4] = count[z % 4] + monitor
        for at, seed in made:
            adjoint_ref[at, :] = seed
        return mass, count

    zeros = [jnp.zeros((8, 128), f32)] * 4
    mass, count = lax.fori_loop(0, NX // 8, block, (list(zeros), list(zeros)))
    send_chip_ref[NX : NX + 8, 0:128] = (mass[0] + mass[1]) + (mass[2] + mass[3])
    send_chip_ref[NX : NX + 8, 128:256] = (count[0] + count[1]) + (count[2] + count[3])
    send_planes(adjoint_ref, send_chip_ref, send_near_ref)


def adjoint_plane(z, next_z, unroll, stage_ref, fields, rg_in_ref, out_ref, rg_ref):
    a_ref, c_ref, ve_ref, vn_ref, co_ref, xb_ref, xf_ref, yb_ref, yf_ref = fields
    at_first, at_last = lane_masks()

    def one(r, j, following, a, next_a, vg, behind, front):
        far_a = [seg_load(a_ref, z, h, r + 2) for h in (0, 1)]
        right, _ = staged(stage_ref, j, False)
        stage_rolls(stage_ref, a_ref, following[0], following[1] + j, j, False)
        vy, back_y, front_y = [], [], []
        for h in (0, 1):
            g = right[h] - a[h]
            vy.append(seg_load(vn_ref, z, h, r) * g)
            back_y.append(seg_load(yb_ref, z, h, r) * g)
            front_y.append(seg_load(yf_ref, z, h, r) * g)
        fl = from_left(front_y, (-6.0 * DIFF_FLAT) * a[0], at_first)
        kr = from_right(back_y, 0.0, at_last)
        new_vg, new_behind, new_front = [], [], []
        for h in (0, 1):
            g = far_a[h] - next_a[h]
            ahead = seg_load(xb_ref, z, h, r + 1) * g + front[h]
            new_vg.append(seg_load(ve_ref, z, h, r + 1) * g)
            new_front.append(seg_load(xf_ref, z, h, r + 1) * g)
            new_behind.append(ahead)
            here = ((back_y[h] - front_y[h]) + (fl[h] - kr[h])) + (behind[h] - ahead) + 6.0 * (vg[h] + vy[h])
            vertical = VERT * vertical_sum(a_ref, z, h, r)
            out = seg_load(co_ref, z, h, r) * a[h] + vertical + (TIME_STEP / 6.0) * here
            seg_store(out_ref, z, h, r, out)
            grad = seg_load(c_ref, z, h, r) * a[h]
            if rg_in_ref is not None:
                grad = grad + seg_load(rg_in_ref, z, h, r)
            seg_store(rg_ref, z, h, r, grad)
        return next_a, far_a, new_vg, new_behind, new_front

    a, next_a, vg, behind, front = [], [], [], [], []
    for h in (0, 1):
        am = seg_load(a_ref, z, h, -1)
        a0 = seg_load(a_ref, z, h, 0)
        a1 = seg_load(a_ref, z, h, 1)
        gm = a0 - am
        g0 = a1 - a0
        a.append(a0)
        next_a.append(a1)
        vg.append(seg_load(ve_ref, z, h, 0) * g0)
        behind.append(seg_load(xb_ref, z, h, 0) * g0 + seg_load(xf_ref, z, h, -1) * gm)
        front.append(seg_load(xf_ref, z, h, 0) * g0)

    def block(i, carry):
        following = next_block(z, next_z, i, unroll)
        for j in range(unroll):
            carry = one(i * unroll + j, j, following, *carry)
        return carry

    lax.fori_loop(0, SEG // unroll, block, (a, next_a, vg, behind, front))
    zero_plane_pads(out_ref, z)


def edge_planes(stage_ref, fields, rg_in_ref, out_ref, rg_ref, send_chip_ref, send_near_ref):
    zero_pads(out_ref)
    stage_first(stage_ref, fields[0], 0, UNROLL, False)
    for z in (0, NZ - 1):
        adjoint_plane(z, NZ - 1, UNROLL, stage_ref, fields, rg_in_ref, out_ref, rg_ref)
    send_planes(out_ref, send_chip_ref, send_near_ref)


def edge_kernel(*refs):
    edge_planes(refs[-1], refs[:9], None, *refs[9:-1])


def turn_kernel(chip_ref, near_ref, ahead_ref, *refs):
    rest, rg_in_ref, (a_ref, out_ref, rg_ref, send_chip_ref, send_near_ref, stage_ref) = refs[:8], refs[8], refs[9:]
    fix_planes(chip_ref, near_ref, ahead_ref, a_ref)
    edge_planes(stage_ref, (a_ref,) + rest, rg_in_ref, out_ref, rg_ref, send_chip_ref, send_near_ref)


def leave_kernel(*refs):
    c_ref, final_ref, sem = refs[11], refs[-3], refs[-1]
    copies = [
        pltpu.make_async_copy(
            c_ref.at[pl.ds(F0 + z * ZP + h * HP, NX), :], final_ref.at[0, z, :, pl.ds(h * 128, 128)], sem.at[z, h]
        )
        for z in range(NZ)
        for h in (0, 1)
    ]
    for copy in copies:
        copy.start()
    inner_kernel(False, *refs[:11], *refs[12:14], refs[-2])
    for copy in copies:
        copy.wait()


def inner_kernel(has_grad, *refs):
    fields, (out_in_ref, rg_in_ref, out_ref, rg_ref, stage_ref) = refs[:9], refs[9:]
    stage_first(stage_ref, fields[0], 1, UNROLL, False)

    def inner(z, unused):
        adjoint_plane(z, z + 1, UNROLL, stage_ref, fields, rg_in_ref if has_grad else None, out_ref, rg_ref)
        return unused

    lax.fori_loop(1, NZ - 1, inner, 0)


def last_kernel(chip_ref, near_ref, prior_ref, ahead_ref, *refs):
    rest, rg_in_ref, (a_ref, out_ref, rg_ref, stage_ref) = refs[:8], refs[8], refs[9:]
    fix_planes(chip_ref, near_ref, ahead_ref, a_ref, prior_ref=prior_ref)
    zero_pads(out_ref)
    stage_first(stage_ref, a_ref, 0, UNROLL, False)
    over_planes(
        lambda z, next_z: adjoint_plane(z, next_z, UNROLL, stage_ref, (a_ref,) + rest, rg_in_ref, out_ref, rg_ref)
    )


def restrict_kernel(share, cells, limit_ref, chip_ref, near_ref, prior_ref, ahead_ref, c0_ref, rg_ref, wells_ref, sums_ref, out_ref, field_ref, wide_ref):
    fix_planes(chip_ref, near_ref, ahead_ref, field_ref, prior_ref=prior_ref)

    def all_of(value):
        return jnp.broadcast_to(jnp.sum(jnp.sum(value, axis=0, keepdims=True), axis=1, keepdims=True), (8, 128))

    count = jnp.maximum(all_of(sums_ref[0:8, 128:256]), 1.0)
    scaled = (all_of(sums_ref[0:8, 0:128]) / count - limit_ref[0]) / SOFT_WIDTH
    small = jnp.exp(-jnp.abs(scaled))
    weight = jnp.where(scaled >= 0.0, 1.0, small) / (1.0 + small) * share
    soft = SOFT_WIDTH * (jnp.maximum(scaled, 0.0) + jnp.log1p(small)) * share
    out_ref[0:2, NX * 16 : NX * 16 + 128] = soft[0:2, :]
    scale = weight * 2.0 / count * (-TIME_STEP * cells)

    def block(j, unused):
        rows = pl.ds(pl.multiple_of(8 * j, 8), 8)
        for h in (0, 1):
            lanes = slice(h * 128, h * 128 + 128)
            for p in (0, 1):
                parts = []
                for z in range(4 * p, 4 * p + 4):
                    at = block_rows(z, h, j)
                    parts.append(wells_ref[z, rows, lanes].astype(f32) * (rg_ref[at, :] + c0_ref[at, :] * field_ref[at, :]))
                wide_ref[p, rows, lanes] = (parts[0] + parts[1]) + (parts[2] + parts[3])
        return unused

    lax.fori_loop(0, NX // 8, block, 0, unroll=2)
    fine = lax.broadcasted_iota(jnp.int32, (NY, 128), 0) // 4
    coarse = lax.broadcasted_iota(jnp.int32, (NY, 128), 1) % 64
    sums = jnp.where(fine == coarse, 1.0, 0.0).astype(f32)
    row = lax.broadcasted_iota(jnp.int32, (NX, 128), 0) % 8
    lane = lax.broadcasted_iota(jnp.int32, (NX, 128), 1)
    own = (row < 4) == (lane < 64)
    for p in (0, 1):
        part = jnp.dot(wide_ref[p], sums, precision=lax.Precision.HIGHEST, preferred_element_type=f32)
        part = jnp.where(own, part, 0.0).reshape(NX // 8, 8, 128).sum(axis=1) * scale[0:1, :]
        for j in range(NX // 8):
            out_ref[p : p + 1, j * 128 : (j + 1) * 128] = part[j : j + 1, :]


def call(kernel, flops, **kwargs):
    return pl.pallas_call(
        kernel,
        compiler_params=pltpu.CompilerParams(vmem_limit_bytes=8 << 20),
        cost_estimate=pl.CostEstimate(flops=flops, bytes_accessed=1 << 20, transcendentals=0),
        **kwargs,
    )


def stage(count):
    return pltpu.VMEM((UNROLL * count * 8, 128), f32)


def dma(*shape):
    return pltpu.SemaphoreType.DMA(shape)


def pair_sum(value, axis, size, step):
    return value + lax.ppermute(value, axis, [(i, i ^ step) for i in range(size)])


def scen_others(value, steps):
    return [lax.ppermute(value, "scen", [(i, i ^ k) for i in range(8)]) for k in steps]


def swap(slab_count, send_chip, send_near):
    near = []
    for i in range(1, slab_count - 1, 2):
        near += [(i, i + 1), (i + 1, i)]
    got_near = lax.ppermute(send_near, "slab", near)
    got_chip = lax.ppermute(send_chip, "slab", [(i, i ^ 1) for i in range(slab_count)])
    return got_chip, got_near


def on_device(start, flow_east, flow_north, wells, monitors, control, multiplier, threshold):
    scen_count = lax.axis_size("scen")
    slab_count = lax.axis_size("slab")
    odd = lax.axis_index("slab") % 2
    in_hbm = functools.partial(pltpu.with_memory_space_constraint, memory_space=pltpu.HBM)

    low, high = start[0, 0], start[0, NZ - 1]
    halos = swap(slab_count, jnp.where(odd == 0, high, low), jnp.where(odd == 0, low, high))
    own = (control + multiplier)[0]
    near = scen_others(own, (1, 2, 3))
    own = (own + near[0]) + (near[1] + near[2])
    consensus = pair_sum(own, "scen", scen_count, 4) / scen_count

    c0, ve, vn, ahead = call(
        first_kernel, 3 << 30,
        in_specs=[HBM] * 3, out_specs=[VM] * 4, out_shape=[FIELD] * 4, scratch_shapes=[stage(4), dma(NZ, 6)],
    )(in_hbm(start), in_hbm(flow_east), in_hbm(flow_north))
    c, send_chip, send_near, co = call(
        rate_kernel, 1 << 28,
        in_specs=[VM] * 6, out_specs=[VM] * 4, out_shape=[FIELD, PLANE, PLANE, FIELD],
        scratch_shapes=[pltpu.VMEM((2, NX, NY), f32)],
        input_output_aliases={2: 0},
    )(*halos, ahead, c0, consensus, wells)
    states = [c0, c]
    slopes = [()]
    for k in range(1, STEPS):
        halos = swap(slab_count, send_chip, send_near)
        ahead, *made = call(step_kernel, 3 << 30, in_specs=[VM] * 4, out_specs=[VM] * 5, out_shape=[FIELD] * 5, scratch_shapes=[stage(4)])(c, ve, vn, co)
        slopes.append(tuple(made))
        if k < STEPS - 1:
            c, send_chip, send_near = call(
                fix_kernel, 1 << 26,
                in_specs=[VM] * 3, out_specs=[VM] * 3, out_shape=[FIELD, PLANE, PLANE],
                input_output_aliases={2: 0},
            )(*halos, ahead)
            states.append(c)
    seed, send_chip, send_near, last = call(
        seed_kernel, 1 << 28,
        in_specs=[VM] * 4, out_specs=[VM] * 4,
        out_shape=[FIELD, jax.ShapeDtypeStruct((NX + 8, NY), f32), PLANE, FIELD],
        input_output_aliases={2: 3},
    )(*halos, ahead, monitors)

    def rest(k):
        return (states[k], ve, vn, co) + slopes[k]

    halos4 = swap(slab_count, send_chip, send_near)
    ahead, grad, send_chip5, send_near5 = call(
        edge_kernel, 1 << 30,
        in_specs=[VM] * 9, out_specs=[VM] * 4, out_shape=[FIELD, FIELD, PLANE, PLANE], scratch_shapes=[stage(2)],
    )(seed, *rest(3))
    halos5 = swap(slab_count, send_chip5, send_near5)
    sums = send_chip[NX:] + halos4[0][NX:]
    sums = pair_sum(sums, "slab", slab_count, 2)
    ahead, grad, final = call(
        leave_kernel, 2 << 30,
        in_specs=[VM] * 12, out_specs=[VM, VM, HBM],
        out_shape=[FIELD, FIELD, jax.ShapeDtypeStruct((1, NZ, NX, NY), f32)],
        input_output_aliases={9: 0, 10: 1}, scratch_shapes=[stage(2), dma(NZ, 2)],
    )(seed, *rest(3), ahead, grad, last)
    adjoint3, ahead, grad, send_chip, send_near = call(
        turn_kernel, 1 << 30,
        in_specs=[VM] * 12, out_specs=[VM] * 5, out_shape=[FIELD, FIELD, FIELD, PLANE, PLANE],
        input_output_aliases={2: 0, 11: 2}, scratch_shapes=[stage(2)],
    )(*halos4, ahead, *rest(2), grad)
    halos6 = swap(slab_count, send_chip, send_near)
    sums = pair_sum(sums, "slab", slab_count, 4)
    ahead, grad = call(
        functools.partial(inner_kernel, True), 2 << 30,
        in_specs=[VM] * 11, out_specs=[VM] * 2, out_shape=[FIELD] * 2,
        input_output_aliases={9: 0, 10: 1}, scratch_shapes=[stage(2)],
    )(adjoint3, *rest(2), ahead, grad)
    sums = pair_sum(sums, "slab", slab_count, 8)
    _, ahead, grad = call(
        last_kernel, 3 << 30,
        in_specs=[VM] * 13, out_specs=[VM] * 3, out_shape=[FIELD] * 3, input_output_aliases={3: 0, 12: 2}, scratch_shapes=[stage(2)],
    )(*halos5, seed, ahead, *rest(1), grad)
    share = 1.0 / ((1.0 - BETA_LEVEL) * scen_count)
    coarse_cells = NZ * slab_count * NX * NY / 64.0
    coarse, _ = call(
        functools.partial(restrict_kernel, share, coarse_cells), 1 << 28,
        in_specs=[pl.BlockSpec(memory_space=pltpu.SMEM)] + [VM] * 8, out_specs=[VM] * 2,
        out_shape=[jax.ShapeDtypeStruct((2, 4096 + 128), f32), FIELD],
        scratch_shapes=[pltpu.VMEM((2, NX, NY), f32)],
        input_output_aliases={4: 1},
    )(threshold, *halos6, adjoint3, ahead, c0, grad, wells, sums)
    near = scen_others(coarse, (1, 2, 3))
    total = (coarse + near[0]) + (near[1] + near[2])
    total = pair_sum(total, "scen", scen_count, 4)
    consensus_next = consensus - total[:, :4096]
    multiplier_next = multiplier + control - consensus_next[None]
    return (final, consensus_next, multiplier_next, threshold + total[0, 4096:4097])


def solution(mesh):
    placed = (
        P("scen", "slab", None, None),
        P("scen", "slab", None, None),
        P("scen", "slab", None, None),
        P("slab", None, None),
        P("slab", None, None),
        P("scen", "slab", None),
        P("scen", "slab", None),
        P(),
    )
    return jax.shard_map(
        on_device,
        mesh=mesh,
        in_specs=placed,
        out_specs=(P("scen", "slab", None, None), P("slab", None), P("scen", "slab", None), P()),
        check_vma=False,
    )
```
